128 devices in a mesh: task: 8 (over x, core), param: 16 (over y, z).
Axes of the slice: x: 4, y: 4, z: 4, core: 2. Of those that a mesh axis runs over, the one named last changes fastest.
Arguments:
- acts: bfloat16 [128, 3584], replicated, may hold values from -6 to 6
- out_grads: bfloat16 [8, 128, 10240], P('task', None, 'param'), may hold values from -12 to 12
- order: int32 [8], replicated, may hold values from 0 to 7, each once
Outputs:
- update: float32 [3584, 10240], P('task', 'param')
- weights: float32 [8], replicated
The draws below stay inside these ranges and needn't reach their ends.
All inputs are finite; a program needn't handle non-finite values.
Results may differ from the reference program's by a relative error of at most 0.0029.
Values may be sent and summed in bfloat16 or wider, within the bound.
No kernel may reach another device: no remote copies, remote signals or barrier semaphores. Data moves between devices by JAX's collectives and lax.ppermute only.
A program may use at most 64 MiB of HBM per device.

```python
import jax
import jax.numpy as jnp
from jax import lax

D = 3584
FFW = 10240
TOK = 128
TASKS = 8
N_PARAM = 16


def draw_out_grads(key, part):
    keys = jax.random.split(jax.random.fold_in(key, 17), 7)
    shared = jnp.clip(jax.random.normal(keys[0], (TOK, FFW), jnp.float32), -4.5, 4.5)
    base = jax.random.uniform(keys[1], (TASKS, 1, 1), jnp.float32, -1.2, 1.2)
    vary = jax.random.uniform(keys[2], (TASKS, 1, 16), jnp.float32, -0.8, 0.8)
    block_ids = jnp.arange(FFW, dtype=jnp.int32) * 16 // FFW
    coupling = base + jnp.take(vary, block_ids, axis=2)
    task_scale = jnp.exp(jax.random.uniform(keys[3], (TASKS, 1, 1), jnp.float32, jnp.log(0.5), jnp.log(2.0)))
    common_col = jnp.exp(jax.random.uniform(keys[4], (1, 1, FFW), jnp.float32, jnp.log(0.3), jnp.log(3.0)))
    own_col = jnp.exp(jax.random.uniform(keys[5], (TASKS, 1, FFW), jnp.float32, jnp.log(0.2), jnp.log(5.0)))
    noise = jnp.clip(jax.random.normal(keys[6], (TASKS, TOK, FFW), jnp.float32), -5.0, 5.0)
    values = task_scale * common_col * own_col * (coupling * shared[None] + noise) / jnp.sqrt(TOK * 1.0)
    return jnp.clip(values, -12.0, 12.0).astype(jnp.bfloat16)


def normal_values(rng, shape, scale, bound, kind=jnp.bfloat16):
    return jnp.clip(scale * jax.random.normal(rng, shape, jnp.float32), -bound, bound).astype(kind)


def setup_inputs(seed: int = 0) -> dict:
    seeds = jax.random.split(jax.random.key(seed), 4)
    acts = normal_values(seeds[0], (TOK, D), 1.0, 6.0)
    out_grads = draw_out_grads(jax.random.fold_in(seeds[3], 71), 0)
    order = jax.random.permutation(seeds[2], TASKS).astype(jnp.int32)
    return dict(acts=acts, out_grads=out_grads, order=order)


def pcgrad_weights(gram, order):
    count = gram.shape[0]
    ids = jnp.arange(count, dtype=jnp.int32)

    def turn(step, mix):
        target = order[step]
        column = gram[:, target]
        onehot = (ids == target).astype(jnp.float32)
        dots = jnp.dot(mix, column, precision=lax.Precision.HIGHEST)
        scale = jnp.sum(column * onehot) + 1e-6
        change = jnp.minimum(dots, 0.0) / scale * (1.0 - onehot)
        return mix - change[:, None] * onehot[None, :]

    mix = lax.fori_loop(0, count, turn, jnp.eye(count, dtype=jnp.float32))
    return jnp.sum(mix, axis=0)


def reference(acts, out_grads, order):
    tasks, tokens, width = out_grads.shape
    block = FFW // N_PARAM
    stacked = out_grads.reshape(tasks, tokens, width // block, block).transpose(2, 0, 1, 3)

    def add(gram, part):
        grads = jnp.einsum("td,ktc->kdc", acts.astype(jnp.float32), part.astype(jnp.float32)).astype(jnp.bfloat16)
        flat = grads.reshape(tasks, -1)
        return gram + jnp.dot(flat, flat.T, preferred_element_type=jnp.float32), None

    gram, _ = lax.scan(add, jnp.zeros((tasks, tasks), jnp.float32), stacked)
    weights = pcgrad_weights(gram, order)
    combined = jnp.einsum("k,ktc->tc", weights, out_grads.astype(jnp.float32), precision=lax.Precision.HIGHEST).astype(jnp.bfloat16)
    update = jnp.dot(acts.T, combined, preferred_element_type=jnp.float32)
    return (update, weights)
```

```python
import functools

import jax
import jax.numpy as jnp
from jax import lax
from jax.experimental import pallas as pl
from jax.experimental.pallas import tpu as pltpu
from jax.sharding import Mesh
from jax.sharding import PartitionSpec as P

TASK = ("task_0", "task_1")
PARAM = ("param_0", "param_1")
LANES = 128


def from_everyone(value, axis):
    devices = lax.axis_size(axis)
    return lax.all_to_all(
        jnp.broadcast_to(value[None], (devices, *value.shape)), axis, 0, 0, tiled=True
    )


def gram_kernel(mine_ref, other_ref, outer_ref, gram_ref, all_ref, rows_ref):
    core = lax.axis_index("task_1")
    chips, tokens, _ = mine_ref.shape
    tasks = 2 * chips
    for chip in range(chips):
        all_ref[pl.ds(2 * chip + core, 1)] = mine_ref[chip : chip + 1]
        all_ref[pl.ds(2 * chip + 1 - core, 1)] = other_ref[chip : chip + 1]
    outer = outer_ref[...]
    for i in range(tasks):
        for j in range(i, tasks):
            pair = lax.dot_general(
                all_ref[i], all_ref[j], (((1,), (1,)), ((), ())), preferred_element_type=jnp.float32
            )
            row = jnp.sum(pair * outer, axis=0, keepdims=True)
            rows_ref[j, i : i + 1, :] = row
            if j > i:
                rows_ref[i, j : j + 1, :] = row
    lane = lax.broadcasted_iota(jnp.int32, (tasks, LANES), 1)
    gram = jnp.zeros((tasks, LANES), jnp.float32)
    for j in range(tasks):
        gram = jnp.where(lane == j, jnp.sum(rows_ref[j], axis=1, keepdims=True), gram)
    gram_ref[...] = gram


def partial_gram(mine, other, outer):
    chips, tokens, width = mine.shape
    tasks = 2 * chips
    flops = tasks * (tasks + 1) * tokens * tokens * width
    return pl.pallas_call(
        gram_kernel,
        out_shape=jax.ShapeDtypeStruct((tasks, LANES), jnp.float32),
        in_specs=[pl.BlockSpec(memory_space=pltpu.VMEM)] * 3,
        out_specs=pl.BlockSpec(memory_space=pltpu.VMEM),
        scratch_shapes=[
            pltpu.VMEM((tasks, tokens, width), jnp.bfloat16),
            pltpu.VMEM((tasks, tasks, LANES), jnp.float32),
        ],
        cost_estimate=pl.CostEstimate(flops=flops, bytes_accessed=0, transcendentals=0),
        compiler_params=pltpu.CompilerParams(vmem_limit_bytes=12 << 20),
        name="partial_gram",
    )(mine, other, outer)


def finish_kernel(
    order_ref, grams_ref, mine_ref, other_ref, acts_ref, update_ref, weights_ref,
    columns_ref, scales_ref, spread_ref, out_ref, sems,
):
    core = lax.axis_index("task_1")
    chips, tokens, width = mine_ref.shape
    tasks = 2 * chips
    lane = lax.broadcasted_iota(jnp.int32, (tasks, LANES), 1)
    sub = lax.broadcasted_iota(jnp.int32, (tasks, LANES), 0)
    gram = grams_ref[0]
    for k in range(1, grams_ref.shape[0]):
        gram = gram + grams_ref[k]
    for j in range(tasks):
        column = jnp.sum(jnp.where(lane == j, gram, 0.0), axis=1, keepdims=True)
        columns_ref[j] = jnp.broadcast_to(column, (tasks, LANES))
        scales_ref[j] = jnp.broadcast_to(column[j : j + 1], (tasks, LANES)) + 1e-06
    mix = (lane == sub).astype(jnp.float32)
    for step in range(tasks):
        target = order_ref[step]
        dots = jnp.sum(mix * columns_ref[target], axis=0, keepdims=True)
        change = jnp.minimum(dots, 0.0) / scales_ref[target]
        mix = mix - jnp.where((sub == target) & (lane != target), change, 0.0)
    weights = jnp.sum(jnp.where(lane < tasks, mix, 0.0), axis=1, keepdims=True)
    spread = jnp.broadcast_to(weights, (tasks, LANES))
    spread_ref[...] = spread
    weights_ref[...] = jnp.sum(jnp.where(lane == sub, spread, 0.0), axis=0, keepdims=True)
    factors = []
    for chip in range(chips):
        factors.append(spread_ref[pl.ds(2 * chip, 1), :])
        factors.append(spread_ref[pl.ds(2 * chip + 1, 1), :])
    copies = []
    for block in range(width // LANES):
        cols = pl.ds(block * LANES, LANES)
        total = jnp.zeros((tokens, LANES), jnp.float32)
        for chip in range(chips):
            a = mine_ref[chip, :, cols]
            b = other_ref[chip, :, cols]
            first = jnp.where(core == 0, a, b).astype(jnp.float32)
            second = jnp.where(core == 0, b, a).astype(jnp.float32)
            total = total + factors[2 * chip] * first
            total = total + factors[2 * chip + 1] * second
        out_ref[:, cols] = lax.dot_general(
            acts_ref[...], total.astype(jnp.bfloat16), (((1,), (0,)), ((), ())),
            preferred_element_type=jnp.float32,
        )
        copy = pltpu.make_async_copy(out_ref.at[:, cols], update_ref.at[:, cols], sems.at[block])
        copy.start()
        copies.append(copy)
    for copy in copies:
        copy.wait()


def finish(order, grams, mine, other, acts_rows):
    chips, tokens, width = mine.shape
    tasks = 2 * chips
    rows = acts_rows.shape[0]
    vmem = pl.BlockSpec(memory_space=pltpu.VMEM)
    return pl.pallas_call(
        finish_kernel,
        out_shape=(
            jax.ShapeDtypeStruct((rows, width), jnp.float32),
            jax.ShapeDtypeStruct((1, LANES), jnp.float32),
        ),
        in_specs=[pl.BlockSpec(memory_space=pltpu.SMEM), vmem, vmem, vmem, vmem],
        out_specs=(pl.BlockSpec(memory_space=pl.ANY), vmem),
        scratch_shapes=[
            pltpu.VMEM((tasks, tasks, LANES), jnp.float32),
            pltpu.VMEM((tasks, tasks, LANES), jnp.float32),
            pltpu.VMEM((tasks, LANES), jnp.float32),
            pltpu.VMEM((rows, width), jnp.float32),
            pltpu.SemaphoreType.DMA((width // LANES,)),
        ],
        cost_estimate=pl.CostEstimate(
            flops=2 * rows * tokens * width, bytes_accessed=4 * rows * width, transcendentals=0
        ),
        compiler_params=pltpu.CompilerParams(vmem_limit_bytes=12 << 20),
        name="finish",
    )(order, grams, mine, other, acts_rows)


def shards(acts, out_grads, order):
    groups = lax.axis_size(TASK)
    group_id = lax.axis_index(TASK)
    part_rows = acts.shape[1] // groups
    mine = from_everyone(out_grads[0], "task_0")
    outer = lax.dot_general(acts, acts, (((1,), (1,)), ((), ())), preferred_element_type=jnp.float32)
    acts_rows = lax.dynamic_slice_in_dim(acts, group_id * part_rows, part_rows, 1).T
    other = lax.ppermute(mine, "task_1", [(0, 1), (1, 0)])
    grams = from_everyone(partial_gram(mine, other, outer), PARAM)
    update, weights = finish(order, grams, mine, other, acts_rows)
    return (update, weights[0, :groups])


def solution(mesh):
    split = Mesh(mesh.devices.reshape(4, 2, 4, 4), ("task_0", "task_1", "param_0", "param_1"))
    placed = (P(), P(TASK, None, PARAM), P())
    return jax.shard_map(
        shards, mesh=split, in_specs=placed, out_specs=(P(TASK, PARAM), P()), check_vma=False
    )
```

```python
import jax
import jax.numpy as jnp
from jax import lax
from jax.experimental import pallas as pl
from jax.experimental.pallas import tpu as pltpu
from jax.sharding import Mesh
from jax.sharding import PartitionSpec as P

TASK = ("task_0", "task_1")
PARAM = ("param_0", "param_1")
LANES = 128
VMEM = pl.BlockSpec(memory_space=pltpu.VMEM)


def params(mib):
    return pltpu.CompilerParams(vmem_limit_bytes=mib << 20)


def chip_at(offset, chips):
    return lax.rem(lax.axis_index("task_0") + offset, chips)


def gram_kernel(*refs):
    chips = (len(refs) - 4) // 2
    mine, other = refs[:chips], refs[chips : 2 * chips]
    outer_ref, row_ref, flat_ref, rows_ref = refs[2 * chips :]
    core = lax.axis_index("task_1")
    tokens = outer_ref.shape[0]
    tasks = 2 * chips
    for offset in range(chips):
        base = chip_at(offset, chips) * 2
        flat_ref[base + core] = mine[offset][...]
        flat_ref[base + 1 - core] = other[offset][...]
    outer = outer_ref[...]
    for i in range(0, tasks, 2):
        for j in range(i, tasks, 2):
            block = lax.dot_general(
                flat_ref[i : i + 2].reshape(2 * tokens, -1), flat_ref[j : j + 2].reshape(2 * tokens, -1),
                (((1,), (1,)), ((), ())), preferred_element_type=jnp.float32,
            )
            for a in range(2):
                for b in range(2):
                    p, q = i + a, j + b
                    if q < p:
                        continue
                    pair = block[tokens * a : tokens * (a + 1), tokens * b : tokens * (b + 1)]
                    row = jnp.sum(pair * outer, axis=0, keepdims=True)
                    rows_ref[q, p : p + 1, :] = row
                    if q > p:
                        rows_ref[p, q : q + 1, :] = row
    lane = lax.broadcasted_iota(jnp.int32, (tasks, LANES), 1)
    sub = lax.broadcasted_iota(jnp.int32, (tasks, LANES), 0)
    gram = jnp.zeros((tasks, LANES), jnp.float32)
    for j in range(tasks):
        total = jnp.sum(rows_ref[j], axis=1, keepdims=True)
        gram = jnp.where(lane == tasks * sub + j, total, gram)
    row_ref[...] = jnp.broadcast_to(jnp.sum(gram, axis=0, keepdims=True), row_ref.shape)


def partial_gram(mine, other, outer, copies):
    tokens, width = mine[0].shape
    tasks = 2 * len(mine)
    flops = tasks * tasks * tokens * tokens * width
    return pl.pallas_call(
        gram_kernel,
        out_shape=jax.ShapeDtypeStruct((copies, LANES), jnp.float32),
        in_specs=[VMEM] * (tasks + 1),
        out_specs=VMEM,
        scratch_shapes=[
            pltpu.VMEM((tasks, tokens, width), jnp.bfloat16),
            pltpu.VMEM((tasks, tasks, LANES), jnp.float32),
        ],
        compiler_params=params(8),
        cost_estimate=pl.CostEstimate(flops=flops, bytes_accessed=0, transcendentals=0),
        name="partial_gram",
    )(*mine, *other, outer)


def finish_kernel(*refs):
    chips = (len(refs) - 9) // 2
    order_ref, grams_ref = refs[:2]
    mine, other = refs[2 : 2 + chips], refs[2 + chips : 2 + 2 * chips]
    acts_ref, update_ref, weights_ref, columns_ref, factor_ref, spread_ref, out_ref, sems = refs[-8:]
    core = lax.axis_index("task_1")
    tokens, width = mine[0].shape
    tasks = 2 * chips
    lane = lax.broadcasted_iota(jnp.int32, (tasks, LANES), 1)
    sub = lax.broadcasted_iota(jnp.int32, (tasks, LANES), 0)
    gram = jnp.sum(grams_ref[...], axis=0, keepdims=True)
    gram = jnp.where((lane >= tasks * sub) & (lane < tasks * sub + tasks), gram, 0.0)
    column_of = lane - tasks * sub
    diagonal = jnp.sum(jnp.where(column_of == sub, gram, 0.0), axis=1, keepdims=True)
    factor_ref[...] = 1.0 / (jnp.broadcast_to(diagonal, (tasks, LANES)) + 1e-06)
    for j in range(tasks):
        column = jnp.sum(jnp.where(column_of == j, gram, 0.0), axis=1, keepdims=True)
        columns_ref[j] = jnp.broadcast_to(column, (tasks, LANES))
    mix = (lane == sub).astype(jnp.float32)
    for step in range(tasks):
        target = order_ref[step]
        dots = jnp.sum(mix * columns_ref[target], axis=0, keepdims=True)
        change = jnp.minimum(dots, 0.0) * factor_ref[pl.ds(target, 1), :]
        mix = mix - jnp.where((sub == target) & (lane != target), change, 0.0)
    weights = jnp.sum(jnp.where(lane < tasks, mix, 0.0), axis=1, keepdims=True)
    spread = jnp.broadcast_to(weights, (tasks, LANES))
    spread_ref[...] = spread
    weights_ref[...] = jnp.sum(jnp.where(lane == sub, spread, 0.0), axis=0)[:tasks]
    terms = []
    for offset in range(chips):
        base = chip_at(offset, chips) * 2
        terms.append((spread_ref[pl.ds(base + core, 1), :], mine[offset]))
        terms.append((spread_ref[pl.ds(base + 1 - core, 1), :], other[offset]))
    copies = []
    for start in range(0, width, 256):
        size = min(256, width - start)
        blocks = []
        for at in range(start, start + size, LANES):
            total = None
            for factor, ref in terms:
                part = factor * ref[:, at : at + LANES].astype(jnp.float32)
                total = part if total is None else total + part
            blocks.append(total.astype(jnp.bfloat16))
        cols = pl.ds(start, size)
        out_ref[:, cols] = lax.dot_general(
            acts_ref[...], jnp.concatenate(blocks, axis=1), (((1,), (0,)), ((), ())),
            preferred_element_type=jnp.float32,
        )
        copy = pltpu.make_async_copy(out_ref.at[:, cols], update_ref.at[:, cols], sems.at[len(copies)])
        copy.start()
        copies.append(copy)
    for copy in copies:
        copy.wait()


def finish(order, grams, mine, other, acts_rows):
    tokens, width = mine[0].shape
    tasks = 2 * len(mine)
    rows = acts_rows.shape[0]
    return pl.pallas_call(
        finish_kernel,
        out_shape=(
            jax.ShapeDtypeStruct((rows, width), jnp.float32),
            jax.ShapeDtypeStruct((tasks,), jnp.float32),
        ),
        in_specs=[pl.BlockSpec(memory_space=pltpu.SMEM)] + [VMEM] * (tasks + 2),
        out_specs=(pl.BlockSpec(memory_space=pl.ANY), VMEM),
        scratch_shapes=[
            pltpu.VMEM((tasks, tasks, LANES), jnp.float32),
            pltpu.VMEM((tasks, LANES), jnp.float32),
            pltpu.VMEM((tasks, LANES), jnp.float32),
            pltpu.VMEM((rows, width), jnp.float32),
            pltpu.SemaphoreType.DMA((pl.cdiv(width, 256),)),
        ],
        compiler_params=params(8),
        cost_estimate=pl.CostEstimate(
            flops=2 * rows * tokens * width, bytes_accessed=4 * rows * width, transcendentals=0
        ),
        name="finish",
    )(order, grams, *mine, *other, acts_rows)


def moved(value, axis, offset):
    count = lax.axis_size(axis)
    return lax.ppermute(value, axis, [((i + offset) % count, i) for i in range(count)])


def shards(acts, out_grads, order):
    tasks = lax.axis_size(TASK)
    task = lax.axis_index(TASK)
    part_rows = acts.shape[1] // tasks
    own = out_grads[0]
    mine = [own] + [moved(own, "task_0", offset) for offset in (1, 2, 3)]
    other = [moved(block, "task_1", 1) for block in mine]
    outer = lax.dot_general(acts, acts, (((1,), (1,)), ((), ())), preferred_element_type=jnp.float32)
    acts_rows = lax.dynamic_slice_in_dim(acts, task * part_rows, part_rows, 1).T
    row = partial_gram(mine, other, outer, lax.axis_size(PARAM))
    row, acts_rows = lax.optimization_barrier((row, acts_rows))
    grams = lax.all_to_all(row, PARAM, 0, 0, tiled=True)
    return finish(order, grams, mine, other, acts_rows)


def solution(mesh):
    split = Mesh(mesh.devices.reshape(4, 2, 4, 4), ("task_0", "task_1", "param_0", "param_1"))
    placed = (P(), P(TASK, None, PARAM), P())
    return jax.shard_map(
        shards, mesh=split, in_specs=placed, out_specs=(P(TASK, PARAM), P()), check_vma=False
    )
```

```python
import jax
import jax.numpy as jnp
from jax import lax
from jax.experimental import pallas as pl
from jax.experimental.pallas import tpu as pltpu
from jax.sharding import Mesh
from jax.sharding import PartitionSpec as P

TASK = ("task_0", "task_1")
PARAM = ("param_0", "param_1")
LANES = 128
VMEM = pl.BlockSpec(memory_space=pltpu.VMEM)


def params(mib):
    return pltpu.CompilerParams(vmem_limit_bytes=mib << 20)


def chip_at(offset, chips):
    return lax.rem(lax.axis_index("task_0") + offset, chips)


def prepare_kernel(
    order_hbm, acts_hbm, own_hbm, outer_ref, rows_ref, turns_ref, own_ref,
    order_ref, acts_ref, both_ref, sems,
):
    copies = [
        pltpu.make_async_copy(acts_hbm, acts_ref, sems.at[0]),
        pltpu.make_async_copy(order_hbm, order_ref, sems.at[1]),
        pltpu.make_async_copy(own_hbm, own_ref, sems.at[2]),
    ]
    for copy in copies:
        copy.start()
    task = lax.axis_index("task_0") * 2 + lax.axis_index("task_1")
    tasks = turns_ref.shape[0]
    span = both_ref.shape[0]
    count = rows_ref.shape[0]
    base = (task // 2) * span
    copies[0].wait()
    outer_ref[...] = lax.dot_general(
        acts_ref[...], acts_ref[...], (((1,), (1,)), ((), ())), preferred_element_type=jnp.float32
    )
    for at in range(0, span, LANES):
        part = acts_ref[:, pl.ds(pl.multiple_of(base + at, LANES), LANES)]
        both_ref[at : at + LANES] = part.T
    rows_ref[...] = both_ref[pl.ds(pl.multiple_of((task % 2) * count, 64), count)]
    copies[1].wait()
    for step in range(tasks):
        turns_ref[step] = jnp.full((tasks, LANES), order_ref[step], jnp.int32)
    copies[2].wait()


def prepare(order, acts, own):
    tokens, depth = acts.shape
    tasks = order.shape[0]
    rows = depth // tasks
    return pl.pallas_call(
        prepare_kernel,
        out_shape=(
            jax.ShapeDtypeStruct((tokens, tokens), jnp.float32),
            jax.ShapeDtypeStruct((rows, tokens), acts.dtype),
            jax.ShapeDtypeStruct((tasks, tasks, LANES), jnp.int32),
            jax.ShapeDtypeStruct(own.shape, own.dtype),
        ),
        in_specs=[pl.BlockSpec(memory_space=pltpu.HBM)] * 3,
        out_specs=(VMEM,) * 4,
        scratch_shapes=[
            pltpu.SMEM((tasks,), jnp.int32),
            pltpu.VMEM(acts.shape, acts.dtype),
            pltpu.VMEM((2 * rows, tokens), acts.dtype),
            pltpu.SemaphoreType.DMA((3,)),
        ],
        compiler_params=params(8),
        cost_estimate=pl.CostEstimate(
            flops=2 * tokens * tokens * depth, bytes_accessed=0, transcendentals=0
        ),
        name="prepare",
    )(order, acts, own)


def place(flat_ref, offset, chips, mine_ref, other_ref):
    core = lax.axis_index("task_1")
    base = chip_at(offset, chips) * 2
    flat_ref[base + core] = mine_ref[...]
    flat_ref[base + 1 - core] = other_ref[...]


def chip_pair(flat_ref, rows_ref, outer, chips, first, second):
    tokens = outer.shape[0]
    first_chip, second_chip = chip_at(first, chips), chip_at(second, chips)
    low = 2 * jnp.minimum(first_chip, second_chip)
    high = 2 * jnp.maximum(first_chip, second_chip)
    block = lax.dot_general(
        flat_ref[pl.ds(low, 2)].reshape(2 * tokens, -1), flat_ref[pl.ds(high, 2)].reshape(2 * tokens, -1),
        (((1,), (1,)), ((), ())), preferred_element_type=jnp.float32,
    )
    for a in range(2):
        for b in range(2):
            if first == second and b < a:
                continue
            pair = block[tokens * a : tokens * (a + 1), tokens * b : tokens * (b + 1)]
            row = jnp.sum(pair * outer, axis=0, keepdims=True)
            rows_ref[high + b, pl.ds(low + a, 1), :] = row
            if first != second or a != b:
                rows_ref[low + a, pl.ds(high + b, 1), :] = row


def early_kernel(m0, m1, m3, o0, o1, o3, outer_ref, flat_ref, rows_ref):
    chips = flat_ref.shape[0] // 2
    for offset, mine_ref, other_ref in ((0, m0, o0), (1, m1, o1), (3, m3, o3)):
        place(flat_ref, offset, chips, mine_ref, other_ref)
    outer = outer_ref[...]
    for first, second in ((0, 0), (1, 1), (3, 3), (0, 1), (0, 3), (1, 3)):
        chip_pair(flat_ref, rows_ref, outer, chips, first, second)


def late_kernel(flat_in_ref, rows_in_ref, m2, o2, outer_ref, row_ref, flat_ref, rows_ref):
    chips = flat_ref.shape[0] // 2
    tasks = 2 * chips
    place(flat_ref, 2, chips, m2, o2)
    outer = outer_ref[...]
    for offset in (2, 0, 1, 3):
        chip_pair(flat_ref, rows_ref, outer, chips, 2, offset)
    lane = lax.broadcasted_iota(jnp.int32, (tasks, LANES), 1)
    sub = lax.broadcasted_iota(jnp.int32, (tasks, LANES), 0)
    gram = jnp.zeros((tasks, LANES), jnp.float32)
    for j in range(tasks):
        total = jnp.sum(rows_ref[j], axis=1, keepdims=True)
        gram = jnp.where(lane == tasks * sub + j, total, gram)
    row_ref[...] = jnp.broadcast_to(jnp.sum(gram, axis=0, keepdims=True), row_ref.shape)


def partial_gram(mine, other, outer, copies):
    tokens, width = mine[0].shape
    tasks = 2 * len(mine)
    pair_flops = 8 * tokens * tokens * width
    held = (
        jax.ShapeDtypeStruct((tasks, tokens, width), jnp.bfloat16),
        jax.ShapeDtypeStruct((tasks, tasks, LANES), jnp.float32),
    )
    flat, rows = pl.pallas_call(
        early_kernel,
        out_shape=held,
        in_specs=[VMEM] * 7,
        out_specs=(VMEM, VMEM),
        compiler_params=params(8),
        cost_estimate=pl.CostEstimate(flops=6 * pair_flops, bytes_accessed=0, transcendentals=0),
        name="early_gram",
    )(mine[0], mine[1], mine[3], other[0], other[1], other[3], outer)
    row, _, _ = pl.pallas_call(
        late_kernel,
        out_shape=(jax.ShapeDtypeStruct((copies, LANES), jnp.float32), *held),
        in_specs=[VMEM] * 5,
        out_specs=(VMEM, VMEM, VMEM),
        input_output_aliases={0: 1, 1: 2},
        compiler_params=params(8),
        cost_estimate=pl.CostEstimate(flops=4 * pair_flops, bytes_accessed=0, transcendentals=0),
        name="late_gram",
    )(flat, rows, mine[2], other[2], outer)
    return row


def finish_kernel(*refs):
    chips = (len(refs) - 9) // 2
    turns_ref, grams_ref = refs[:2]
    mine, other = refs[2 : 2 + chips], refs[2 + chips : 2 + 2 * chips]
    acts_ref, update_ref, weights_ref, spread_ref, flat_ref, out_ref, sems = refs[-7:]
    core = lax.axis_index("task_1")
    _, width = mine[0].shape
    tasks = 2 * chips
    lane = lax.broadcasted_iota(jnp.int32, (tasks, LANES), 1)
    sub = lax.broadcasted_iota(jnp.int32, (tasks, LANES), 0)
    column_of = lane - tasks * sub
    gram = jnp.sum(grams_ref[...], axis=0, keepdims=True)
    gram = jnp.broadcast_to(gram, (tasks, LANES))
    mix = (lane == sub).astype(jnp.float32)
    steps = []
    for step in range(tasks):
        target = turns_ref[step]
        column = jnp.sum(jnp.where(column_of == target, gram, 0.0), axis=1, keepdims=True)
        column = jnp.broadcast_to(column, (tasks, LANES))
        scale = jnp.sum(jnp.where(sub == target, column, 0.0), axis=0, keepdims=True) + 1e-06
        steps.append((column, 1.0 / scale, (sub == target) & (lane != target)))
    for column, factor, touched in steps:
        dots = jnp.sum(mix * column, axis=0, keepdims=True)
        change = jnp.minimum(dots, 0.0) * factor
        mix = mix - jnp.where(touched, change, 0.0)
    weights = jnp.sum(jnp.where(lane < tasks, mix, 0.0), axis=1, keepdims=True)
    spread = jnp.broadcast_to(weights, (tasks, LANES))
    spread_ref[...] = spread
    flat_ref[...] = jnp.sum(jnp.where(lane == sub, spread, 0.0), axis=0)[:tasks]
    copies = [pltpu.make_async_copy(flat_ref, weights_ref, sems.at[0])]
    copies[0].start()
    terms = []
    for offset in range(chips):
        base = chip_at(offset, chips) * 2
        terms.append((spread_ref[pl.ds(base + core, 1), :], mine[offset]))
        terms.append((spread_ref[pl.ds(base + 1 - core, 1), :], other[offset]))
    for start in range(0, width, 256):
        size = min(256, width - start)
        blocks = []
        for at in range(start, start + size, LANES):
            total = None
            for factor, ref in terms:
                part = factor * ref[:, at : at + LANES].astype(jnp.float32)
                total = part if total is None else total + part
            blocks.append(total.astype(jnp.bfloat16))
        cols = pl.ds(start, size)
        out_ref[:, cols] = lax.dot_general(
            acts_ref[...], jnp.concatenate(blocks, axis=1), (((1,), (0,)), ((), ())),
            preferred_element_type=jnp.float32,
        )
        copy = pltpu.make_async_copy(out_ref.at[:, cols], update_ref.at[:, cols], sems.at[len(copies)])
        copy.start()
        copies.append(copy)
    for copy in copies:
        copy.wait()


def finish(turns, grams, mine, other, acts_rows):
    tokens, width = mine[0].shape
    tasks = 2 * len(mine)
    rows = acts_rows.shape[0]
    return pl.pallas_call(
        finish_kernel,
        out_shape=(
            jax.ShapeDtypeStruct((rows, width), jnp.float32),
            jax.ShapeDtypeStruct((tasks,), jnp.float32),
        ),
        in_specs=[VMEM] * (tasks + 3),
        out_specs=(pl.BlockSpec(memory_space=pl.ANY),) * 2,
        scratch_shapes=[
            pltpu.VMEM((tasks, LANES), jnp.float32),
            pltpu.VMEM((tasks,), jnp.float32),
            pltpu.VMEM((rows, width), jnp.float32),
            pltpu.SemaphoreType.DMA((1 + pl.cdiv(width, 256),)),
        ],
        compiler_params=params(8),
        cost_estimate=pl.CostEstimate(
            flops=2 * rows * tokens * width, bytes_accessed=4 * rows * width, transcendentals=0
        ),
        name="finish",
    )(turns, grams, *mine, *other, acts_rows)


def moved(value, axis, offset):
    count = lax.axis_size(axis)
    return lax.ppermute(value, axis, [((i + offset) % count, i) for i in range(count)])


def shards(acts, out_grads, order):
    mine, other = [out_grads[0]], []
    for offset in (1, 2, 3):
        mine.append(moved(mine[0], "task_0", offset))
    for offset in (0, 1, 2, 3):
        other.append(moved(mine[offset], "task_1", 1))
    outer, acts_rows, turns, held = prepare(order, acts, mine[0])
    mine[0] = held
    row = partial_gram(mine, other, outer, lax.axis_size(PARAM))
    grams = lax.all_to_all(row, PARAM, 0, 0, tiled=True)
    return finish(turns, grams, mine, other, acts_rows)


def solution(mesh):
    split = Mesh(mesh.devices.reshape(4, 2, 4, 4), ("task_0", "task_1", "param_0", "param_1"))
    placed = (P(), P(TASK, None, PARAM), P())
    return jax.shard_map(
        shards, mesh=split, in_specs=placed, out_specs=(P(TASK, PARAM), P()), check_vma=False
    )
```

```python
import jax
import jax.numpy as jnp
from jax import lax
from jax.experimental import pallas as pl
from jax.experimental.pallas import tpu as pltpu
from jax.sharding import Mesh
from jax.sharding import PartitionSpec as P

TASK = ("task_0", "task_1")
PARAM = ("param_0", "param_1")
LANES = 128
ORDER = (3, 1, 2)
FLIP = (2,)
VMEM = pl.BlockSpec(memory_space=pltpu.VMEM)


def params(mib):
    return pltpu.CompilerParams(vmem_limit_bytes=mib << 20)


def chip_at(offset):
    return lax.bitwise_xor(lax.axis_index("task_0"), offset)


def prepare_kernel(
    order_hbm, acts_hbm, own_hbm, outer_ref, rows_ref, turns_ref, own_ref,
    order_ref, acts_ref, both_ref, sems,
):
    copies = [
        pltpu.make_async_copy(acts_hbm, acts_ref, sems.at[0]),
        pltpu.make_async_copy(order_hbm, order_ref, sems.at[1]),
        pltpu.make_async_copy(own_hbm, own_ref, sems.at[2]),
    ]
    for copy in copies:
        copy.start()
    task = lax.axis_index("task_0") * 2 + lax.axis_index("task_1")
    tasks = turns_ref.shape[0]
    span = both_ref.shape[0]
    count = rows_ref.shape[0]
    base = (task // 2) * span
    copies[0].wait()
    outer_ref[...] = lax.dot_general(
        acts_ref[...], acts_ref[...], (((1,), (1,)), ((), ())), preferred_element_type=jnp.float32
    )
    for at in range(0, span, LANES):
        part = acts_ref[:, pl.ds(pl.multiple_of(base + at, LANES), LANES)]
        both_ref[at : at + LANES] = part.T
    rows_ref[...] = both_ref[pl.ds(pl.multiple_of((task % 2) * count, 64), count)]
    copies[1].wait()
    for step in range(tasks):
        turns_ref[step] = jnp.full((tasks, LANES), order_ref[step], jnp.int32)
    copies[2].wait()


def prepare(order, acts, own):
    tokens, depth = acts.shape
    tasks = order.shape[0]
    rows = depth // tasks
    return pl.pallas_call(
        prepare_kernel,
        out_shape=(
            jax.ShapeDtypeStruct((tokens, tokens), jnp.float32),
            jax.ShapeDtypeStruct((rows, tokens), acts.dtype),
            jax.ShapeDtypeStruct((tasks, tasks, LANES), jnp.int32),
            jax.ShapeDtypeStruct(own.shape, own.dtype),
        ),
        in_specs=[pl.BlockSpec(memory_space=pltpu.HBM)] * 3,
        out_specs=(VMEM,) * 4,
        scratch_shapes=[
            pltpu.SMEM((tasks,), jnp.int32),
            pltpu.VMEM(acts.shape, acts.dtype),
            pltpu.VMEM((2 * rows, tokens), acts.dtype),
            pltpu.SemaphoreType.DMA((3,)),
        ],
        compiler_params=params(8),
        cost_estimate=pl.CostEstimate(
            flops=2 * tokens * tokens * depth, bytes_accessed=0, transcendentals=0
        ),
        name="prepare",
    )(order, acts, own)


def place(flat_ref, offset, mine_ref, other_ref):
    core = lax.axis_index("task_1")
    base = chip_at(offset) * 2
    side = 1 - core if offset in FLIP else core
    flat_ref[base + side] = mine_ref[...]
    flat_ref[base + 1 - side] = other_ref[...]


def chip_pair(flat_ref, rows_ref, outer, first, second):
    tokens = outer.shape[0]
    first_chip, second_chip = chip_at(first), chip_at(second)
    low = 2 * jnp.minimum(first_chip, second_chip)
    high = 2 * jnp.maximum(first_chip, second_chip)
    block = lax.dot_general(
        flat_ref[pl.ds(low, 2)].reshape(2 * tokens, -1), flat_ref[pl.ds(high, 2)].reshape(2 * tokens, -1),
        (((1,), (1,)), ((), ())), preferred_element_type=jnp.float32,
    )
    for a in range(2):
        for b in range(2):
            if first == second and b < a:
                continue
            pair = block[tokens * a : tokens * (a + 1), tokens * b : tokens * (b + 1)]
            row = jnp.sum(pair * outer, axis=0, keepdims=True)
            rows_ref[high + b, pl.ds(low + a, 1), :] = row
            if first != second or a != b:
                rows_ref[low + a, pl.ds(high + b, 1), :] = row


def early_kernel(*refs):
    outer_ref, flat_ref, rows_ref = refs[-3:]
    held = (0, *ORDER[:-1])
    for at, offset in enumerate(held):
        place(flat_ref, offset, refs[2 * at], refs[2 * at + 1])
    outer = outer_ref[...]
    for at, second in enumerate(held):
        for first in held[: at + 1]:
            chip_pair(flat_ref, rows_ref, outer, first, second)


def late_kernel(flat_in_ref, rows_in_ref, m2, o2, outer_ref, row_ref, flat_ref, rows_ref):
    chips = flat_ref.shape[0] // 2
    tasks = 2 * chips
    last = ORDER[-1]
    place(flat_ref, last, m2, o2)
    outer = outer_ref[...]
    for offset in (last, 0, *ORDER[:-1]):
        chip_pair(flat_ref, rows_ref, outer, last, offset)
    lane = lax.broadcasted_iota(jnp.int32, (tasks, LANES), 1)
    sub = lax.broadcasted_iota(jnp.int32, (tasks, LANES), 0)
    gram = jnp.zeros((tasks, LANES), jnp.float32)
    for j in range(tasks):
        total = jnp.sum(rows_ref[j], axis=1, keepdims=True)
        gram = jnp.where(lane == tasks * sub + j, total, gram)
    row_ref[...] = jnp.broadcast_to(jnp.sum(gram, axis=0, keepdims=True), row_ref.shape)


def partial_gram(mine, other, outer, copies):
    tokens, width = mine[0].shape
    tasks = 2 * len(mine)
    pair_flops = 8 * tokens * tokens * width
    held = (
        jax.ShapeDtypeStruct((tasks, tokens, width), jnp.bfloat16),
        jax.ShapeDtypeStruct((tasks, tasks, LANES), jnp.float32),
    )
    flat, rows = pl.pallas_call(
        early_kernel,
        out_shape=held,
        in_specs=[VMEM] * 7,
        out_specs=(VMEM, VMEM),
        compiler_params=params(8),
        cost_estimate=pl.CostEstimate(flops=6 * pair_flops, bytes_accessed=0, transcendentals=0),
        name="early_gram",
    )(*(block[offset] for offset in (0, *ORDER[:-1]) for block in (mine, other)), outer)
    row, _, _ = pl.pallas_call(
        late_kernel,
        out_shape=(jax.ShapeDtypeStruct((copies, LANES), jnp.float32), *held),
        in_specs=[VMEM] * 5,
        out_specs=(VMEM, VMEM, VMEM),
        input_output_aliases={0: 1, 1: 2},
        compiler_params=params(8),
        cost_estimate=pl.CostEstimate(flops=4 * pair_flops, bytes_accessed=0, transcendentals=0),
        name="late_gram",
    )(flat, rows, mine[ORDER[-1]], other[ORDER[-1]], outer)
    return row


def finish_kernel(*refs):
    chips = (len(refs) - 9) // 2
    turns_ref, grams_ref = refs[:2]
    mine, other = refs[2 : 2 + chips], refs[2 + chips : 2 + 2 * chips]
    acts_ref, update_ref, weights_ref, spread_ref, flat_ref, out_ref, sems = refs[-7:]
    core = lax.axis_index("task_1")
    _, width = mine[0].shape
    tasks = 2 * chips
    lane = lax.broadcasted_iota(jnp.int32, (tasks, LANES), 1)
    sub = lax.broadcasted_iota(jnp.int32, (tasks, LANES), 0)
    column_of = lane - tasks * sub
    gram = jnp.sum(grams_ref[...], axis=0, keepdims=True)
    gram = jnp.broadcast_to(gram, (tasks, LANES))
    mix = (lane == sub).astype(jnp.float32)
    steps = []
    for step in range(tasks):
        target = turns_ref[step]
        column = jnp.sum(jnp.where(column_of == target, gram, 0.0), axis=1, keepdims=True)
        column = jnp.broadcast_to(column, (tasks, LANES))
        scale = jnp.sum(jnp.where(sub == target, column, 0.0), axis=0, keepdims=True) + 1e-06
        steps.append((column, 1.0 / scale, (sub == target) & (lane != target)))
    for column, factor, touched in steps:
        dots = jnp.sum(mix * column, axis=0, keepdims=True)
        change = jnp.minimum(dots, 0.0) * factor
        mix = mix - jnp.where(touched, change, 0.0)
    weights = jnp.sum(jnp.where(lane < tasks, mix, 0.0), axis=1, keepdims=True)
    spread = jnp.broadcast_to(weights, (tasks, LANES))
    spread_ref[...] = spread
    flat_ref[...] = jnp.sum(jnp.where(lane == sub, spread, 0.0), axis=0)[:tasks]
    copies = [pltpu.make_async_copy(flat_ref, weights_ref, sems.at[0])]
    copies[0].start()
    terms = []
    for offset in range(chips):
        base = chip_at(offset) * 2
        side = 1 - core if offset in FLIP else core
        terms.append((spread_ref[pl.ds(base + side, 1), :], mine[offset]))
        terms.append((spread_ref[pl.ds(base + 1 - side, 1), :], other[offset]))
    for start in range(0, width, 256):
        size = min(256, width - start)
        blocks = []
        for at in range(start, start + size, LANES):
            total = None
            for factor, ref in terms:
                part = factor * ref[:, at : at + LANES].astype(jnp.float32)
                total = part if total is None else total + part
            blocks.append(total.astype(jnp.bfloat16))
        cols = pl.ds(start, size)
        out_ref[:, cols] = lax.dot_general(
            acts_ref[...], jnp.concatenate(blocks, axis=1), (((1,), (0,)), ((), ())),
            preferred_element_type=jnp.float32,
        )
        copy = pltpu.make_async_copy(out_ref.at[:, cols], update_ref.at[:, cols], sems.at[len(copies)])
        copy.start()
        copies.append(copy)
    for copy in copies:
        copy.wait()


def finish(turns, grams, mine, other, acts_rows):
    tokens, width = mine[0].shape
    tasks = 2 * len(mine)
    rows = acts_rows.shape[0]
    return pl.pallas_call(
        finish_kernel,
        out_shape=(
            jax.ShapeDtypeStruct((rows, width), jnp.float32),
            jax.ShapeDtypeStruct((tasks,), jnp.float32),
        ),
        in_specs=[VMEM] * (tasks + 3),
        out_specs=(pl.BlockSpec(memory_space=pl.ANY),) * 2,
        scratch_shapes=[
            pltpu.VMEM((tasks, LANES), jnp.float32),
            pltpu.VMEM((tasks,), jnp.float32),
            pltpu.VMEM((rows, width), jnp.float32),
            pltpu.SemaphoreType.DMA((1 + pl.cdiv(width, 256),)),
        ],
        compiler_params=params(8),
        cost_estimate=pl.CostEstimate(
            flops=2 * rows * tokens * width, bytes_accessed=4 * rows * width, transcendentals=0
        ),
        name="finish",
    )(turns, grams, *mine, *other, acts_rows)


def moved(value, offset):
    chips = lax.axis_size("task_0")
    pairs = [
        (2 * (chip ^ offset) + (1 - core if offset in FLIP else core), 2 * chip + core)
        for chip in range(chips)
        for core in range(2)
    ]
    return lax.ppermute(value, TASK, pairs)


def shards(acts, out_grads, order):
    mine, other = [out_grads[0]], []
    for offset in (1, 2, 3):
        mine.append(moved(mine[0], offset))
    for offset in (0, 1, 2, 3):
        other.append(lax.ppermute(mine[offset], "task_1", [(0, 1), (1, 0)]))
    outer, acts_rows, turns, held = prepare(order, acts, mine[0])
    mine[0] = held
    row = partial_gram(mine, other, outer, lax.axis_size(PARAM))
    grams = lax.all_to_all(row, PARAM, 0, 0, tiled=True, axis_index_groups=[[10, 0, 1, 2, 3, 4, 5, 6, 7, 8, 9, 11, 12, 13, 14, 15]])
    return finish(turns, grams, mine, other, acts_rows)


def solution(mesh):
    split = Mesh(mesh.devices.reshape(4, 2, 4, 4), ("task_0", "task_1", "param_0", "param_1"))
    placed = (P(), P(TASK, None, PARAM), P())
    return jax.shard_map(
        shards, mesh=split, in_specs=placed, out_specs=(P(TASK, PARAM), P()), check_vma=False
    )
```

```python
import jax
import jax.numpy as jnp
from jax import lax
from jax.experimental import pallas as pl
from jax.experimental.pallas import tpu as pltpu
from jax.sharding import Mesh
from jax.sharding import PartitionSpec as P

TASK = ("task_0", "task_1")
PARAM = ("param_0", "param_1")
LANES = 128
ORDER = (3, 1, 2)
FLIP = (2,)
VMEM = pl.BlockSpec(memory_space=pltpu.VMEM)


def params(mib):
    return pltpu.CompilerParams(vmem_limit_bytes=mib << 20)


def chip_at(offset):
    return lax.bitwise_xor(lax.axis_index("task_0"), offset)


def prepare_kernel(
    order_hbm, acts_hbm, own_hbm, outer_ref, rows_ref, turns_ref, own_ref,
    order_ref, acts_ref, both_ref, sems,
):
    copies = [
        pltpu.make_async_copy(acts_hbm, acts_ref, sems.at[0]),
        pltpu.make_async_copy(order_hbm, order_ref, sems.at[1]),
        pltpu.make_async_copy(own_hbm, own_ref, sems.at[2]),
    ]
    for copy in copies:
        copy.start()
    task = lax.axis_index("task_0") * 2 + lax.axis_index("task_1")
    tasks = turns_ref.shape[0]
    span = both_ref.shape[0]
    count = rows_ref.shape[0]
    base = (task // 2) * span
    copies[0].wait()
    outer_ref[...] = lax.dot_general(
        acts_ref[...], acts_ref[...], (((1,), (1,)), ((), ())), preferred_element_type=jnp.float32
    )
    for at in range(0, span, LANES):
        part = acts_ref[:, pl.ds(pl.multiple_of(base + at, LANES), LANES)]
        both_ref[at : at + LANES] = part.T
    rows_ref[...] = both_ref[pl.ds(pl.multiple_of((task % 2) * count, 64), count)]
    copies[1].wait()
    for step in range(tasks):
        turns_ref[step] = jnp.full((tasks, LANES), order_ref[step], jnp.int32)
    copies[2].wait()


def prepare(order, acts, own):
    tokens, depth = acts.shape
    tasks = order.shape[0]
    rows = depth // tasks
    return pl.pallas_call(
        prepare_kernel,
        out_shape=(
            jax.ShapeDtypeStruct((tokens, tokens), jnp.float32),
            jax.ShapeDtypeStruct((rows, tokens), acts.dtype),
            jax.ShapeDtypeStruct((tasks, tasks, LANES), jnp.int32),
            jax.ShapeDtypeStruct(own.shape, own.dtype),
        ),
        in_specs=[pl.BlockSpec(memory_space=pltpu.HBM)] * 3,
        out_specs=(VMEM,) * 4,
        scratch_shapes=[
            pltpu.SMEM((tasks,), jnp.int32),
            pltpu.VMEM(acts.shape, acts.dtype),
            pltpu.VMEM((2 * rows, tokens), acts.dtype),
            pltpu.SemaphoreType.DMA((3,)),
        ],
        compiler_params=params(8),
        cost_estimate=pl.CostEstimate(
            flops=2 * tokens * tokens * depth, bytes_accessed=0, transcendentals=0
        ),
        name="prepare",
    )(order, acts, own)


def place(flat_ref, offset, mine_ref, other_ref):
    core = lax.axis_index("task_1")
    base = chip_at(offset) * 2
    side = 1 - core if offset in FLIP else core
    flat_ref[base + side] = mine_ref[...]
    flat_ref[base + 1 - side] = other_ref[...]


def chip_pair(flat_ref, rows_ref, outer, first, second):
    tokens = outer.shape[0]
    first_chip, second_chip = chip_at(first), chip_at(second)
    low = 2 * jnp.minimum(first_chip, second_chip)
    high = 2 * jnp.maximum(first_chip, second_chip)
    block = lax.dot_general(
        flat_ref[pl.ds(low, 2)].reshape(2 * tokens, -1), flat_ref[pl.ds(high, 2)].reshape(2 * tokens, -1),
        (((1,), (1,)), ((), ())), preferred_element_type=jnp.float32,
    )
    for a in range(2):
        for b in range(2):
            if first == second and b < a:
                continue
            pair = block[tokens * a : tokens * (a + 1), tokens * b : tokens * (b + 1)]
            row = jnp.sum(pair * outer, axis=0, keepdims=True)
            rows_ref[high + b, pl.ds(low + a, 1), :] = row
            if first != second or a != b:
                rows_ref[low + a, pl.ds(high + b, 1), :] = row


def early_kernel(*refs):
    outer_ref, flat_ref, rows_ref = refs[-3:]
    held = (0, *ORDER[:-1])
    for at, offset in enumerate(held):
        place(flat_ref, offset, refs[2 * at], refs[2 * at + 1])
    outer = outer_ref[...]
    for at, second in enumerate(held):
        for first in held[: at + 1]:
            chip_pair(flat_ref, rows_ref, outer, first, second)


def late_kernel(flat_in_ref, rows_in_ref, m2, o2, outer_ref, row_ref, flat_ref, rows_ref):
    chips = flat_ref.shape[0] // 2
    tasks = 2 * chips
    last = ORDER[-1]
    place(flat_ref, last, m2, o2)
    outer = outer_ref[...]
    for offset in (0, *ORDER[:-1], last):
        chip_pair(flat_ref, rows_ref, outer, last, offset)
    lane = lax.broadcasted_iota(jnp.int32, (tasks, LANES), 1)
    sub = lax.broadcasted_iota(jnp.int32, (tasks, LANES), 0)
    gram = jnp.zeros((tasks, LANES), jnp.float32)
    for j in range(tasks):
        total = jnp.sum(rows_ref[j], axis=1, keepdims=True)
        gram = jnp.where(lane == tasks * sub + j, total, gram)
    row_ref[...] = jnp.broadcast_to(jnp.sum(gram, axis=0, keepdims=True), row_ref.shape)


def partial_gram(mine, other, outer, copies):
    tokens, width = mine[0].shape
    tasks = 2 * len(mine)
    pair_flops = 8 * tokens * tokens * width
    held = (
        jax.ShapeDtypeStruct((tasks, tokens, width), jnp.bfloat16),
        jax.ShapeDtypeStruct((tasks, tasks, LANES), jnp.float32),
    )
    flat, rows = pl.pallas_call(
        early_kernel,
        out_shape=held,
        in_specs=[VMEM] * 7,
        out_specs=(VMEM, VMEM),
        compiler_params=params(8),
        cost_estimate=pl.CostEstimate(flops=6 * pair_flops, bytes_accessed=0, transcendentals=0),
        name="early_gram",
    )(*(block[offset] for offset in (0, *ORDER[:-1]) for block in (mine, other)), outer)
    row, _, _ = pl.pallas_call(
        late_kernel,
        out_shape=(jax.ShapeDtypeStruct((copies, LANES), jnp.float32), *held),
        in_specs=[VMEM] * 5,
        out_specs=(VMEM, VMEM, VMEM),
        input_output_aliases={0: 1, 1: 2},
        compiler_params=params(8),
        cost_estimate=pl.CostEstimate(flops=4 * pair_flops, bytes_accessed=0, transcendentals=0),
        name="late_gram",
    )(flat, rows, mine[ORDER[-1]], other[ORDER[-1]], outer)
    return row


def finish_kernel(*refs):
    chips = (len(refs) - 9) // 2
    turns_ref, grams_ref = refs[:2]
    mine, other = refs[2 : 2 + chips], refs[2 + chips : 2 + 2 * chips]
    acts_ref, update_ref, weights_ref, spread_ref, flat_ref, out_ref, sems = refs[-7:]
    core = lax.axis_index("task_1")
    _, width = mine[0].shape
    tasks = 2 * chips
    lane = lax.broadcasted_iota(jnp.int32, (tasks, LANES), 1)
    sub = lax.broadcasted_iota(jnp.int32, (tasks, LANES), 0)
    column_of = lane - tasks * sub
    gram = jnp.sum(grams_ref[...], axis=0, keepdims=True)
    gram = jnp.broadcast_to(gram, (tasks, LANES))
    mix = (lane == sub).astype(jnp.float32)
    steps = []
    for step in range(tasks):
        target = turns_ref[step]
        column = jnp.sum(jnp.where(column_of == target, gram, 0.0), axis=1, keepdims=True)
        column = jnp.broadcast_to(column, (tasks, LANES))
        scale = jnp.sum(jnp.where(sub == target, column, 0.0), axis=0, keepdims=True) + 1e-06
        steps.append((column, 1.0 / scale, (sub == target) & (lane != target)))
    for column, factor, touched in steps:
        dots = jnp.sum(mix * column, axis=0, keepdims=True)
        change = jnp.minimum(dots, 0.0) * factor
        mix = mix - jnp.where(touched, change, 0.0)
    weights = jnp.sum(jnp.where(lane < tasks, mix, 0.0), axis=1, keepdims=True)
    spread = jnp.broadcast_to(weights, (tasks, LANES))
    spread_ref[...] = spread
    flat_ref[...] = jnp.sum(jnp.where(lane == sub, spread, 0.0), axis=0)[:tasks]
    copies = [pltpu.make_async_copy(flat_ref, weights_ref, sems.at[0])]
    terms = []
    for offset in range(chips):
        base = chip_at(offset) * 2
        side = 1 - core if offset in FLIP else core
        terms.append((spread_ref[pl.ds(base + side, 1), :], mine[offset]))
        terms.append((spread_ref[pl.ds(base + 1 - side, 1), :], other[offset]))
    for start in range(0, width, 256):
        size = min(256, width - start)
        blocks = []
        for at in range(start, start + size, LANES):
            total = None
            for factor, ref in terms:
                part = factor * ref[:, at : at + LANES].astype(jnp.float32)
                total = part if total is None else total + part
            blocks.append(total.astype(jnp.bfloat16))
        cols = pl.ds(start, size)
        out_ref[:, cols] = lax.dot_general(
            acts_ref[...], jnp.concatenate(blocks, axis=1), (((1,), (0,)), ((), ())),
            preferred_element_type=jnp.float32,
        )
        copy = pltpu.make_async_copy(out_ref.at[:, cols], update_ref.at[:, cols], sems.at[len(copies)])
        copy.start()
        copies.append(copy)
    copies[0].start()
    for copy in copies:
        copy.wait()


def finish(turns, grams, mine, other, acts_rows):
    tokens, width = mine[0].shape
    tasks = 2 * len(mine)
    rows = acts_rows.shape[0]
    return pl.pallas_call(
        finish_kernel,
        out_shape=(
            jax.ShapeDtypeStruct((rows, width), jnp.float32),
            jax.ShapeDtypeStruct((tasks,), jnp.float32),
        ),
        in_specs=[VMEM] * (tasks + 3),
        out_specs=(pl.BlockSpec(memory_space=pl.ANY),) * 2,
        scratch_shapes=[
            pltpu.VMEM((tasks, LANES), jnp.float32),
            pltpu.VMEM((tasks,), jnp.float32),
            pltpu.VMEM((rows, width), jnp.float32),
            pltpu.SemaphoreType.DMA((1 + pl.cdiv(width, 256),)),
        ],
        compiler_params=params(8),
        cost_estimate=pl.CostEstimate(
            flops=2 * rows * tokens * width, bytes_accessed=4 * rows * width, transcendentals=0
        ),
        name="finish",
    )(turns, grams, *mine, *other, acts_rows)


def moved(value, offset):
    chips = lax.axis_size("task_0")
    pairs = [
        (2 * (chip ^ offset) + (1 - core if offset in FLIP else core), 2 * chip + core)
        for chip in range(chips)
        for core in range(2)
    ]
    return lax.ppermute(value, TASK, pairs)


def farthest_first():
    rows, columns = lax.axis_size(PARAM[0]), lax.axis_size(PARAM[1])
    farthest = rows // 2 * columns + columns // 2
    return [farthest] + [chip for chip in range(rows * columns) if chip != farthest]


def shards(acts, out_grads, order):
    mine, other = [out_grads[0]], []
    for offset in (1, 2, 3):
        mine.append(moved(mine[0], offset))
    for offset in (0, 1, 2, 3):
        other.append(lax.ppermute(mine[offset], "task_1", [(0, 1), (1, 0)]))
    outer, acts_rows, turns, held = prepare(order, acts, mine[0])
    mine[0] = held
    row = partial_gram(mine, other, outer, lax.axis_size(PARAM))
    grams = lax.all_to_all(row, PARAM, 0, 0, tiled=True, axis_index_groups=[farthest_first()])
    return finish(turns, grams, mine, other, acts_rows)


def solution(mesh):
    split = Mesh(mesh.devices.reshape(4, 2, 4, 4), ("task_0", "task_1", "param_0", "param_1"))
    placed = (P(), P(TASK, None, PARAM), P())
    return jax.shard_map(
        shards, mesh=split, in_specs=placed, out_specs=(P(TASK, PARAM), P()), check_vma=False
    )
```

```python
import jax
import jax.numpy as jnp
from jax import lax
from jax.experimental import pallas as pl
from jax.experimental.pallas import tpu as pltpu
from jax.sharding import Mesh
from jax.sharding import PartitionSpec as P

TASK = ("task_0", "task_1")
PARAM = ("param_0", "param_1")
LANES = 128
ORDER = (3, 1, 2)
FLIP = (2,)
VMEM = pl.BlockSpec(memory_space=pltpu.VMEM)


def params(mib):
    return pltpu.CompilerParams(vmem_limit_bytes=mib << 20)


def chip_at(offset):
    return lax.bitwise_xor(lax.axis_index("task_0"), offset)


def prepare_kernel(
    order_hbm, acts_hbm, own_hbm, outer_ref, rows_ref, turns_ref, own_ref,
    order_ref, acts_ref, both_ref, sems,
):
    copies = [
        pltpu.make_async_copy(acts_hbm, acts_ref, sems.at[0]),
        pltpu.make_async_copy(order_hbm, order_ref, sems.at[1]),
        pltpu.make_async_copy(own_hbm, own_ref, sems.at[2]),
    ]
    for copy in copies:
        copy.start()
    task = lax.axis_index("task_0") * 2 + lax.axis_index("task_1")
    tasks = turns_ref.shape[0]
    span = both_ref.shape[0]
    count = rows_ref.shape[0]
    base = (task // 2) * span
    copies[0].wait()
    outer_ref[...] = lax.dot_general(
        acts_ref[...], acts_ref[...], (((1,), (1,)), ((), ())), preferred_element_type=jnp.float32
    )
    for at in range(0, span, LANES):
        part = acts_ref[:, pl.ds(pl.multiple_of(base + at, LANES), LANES)]
        both_ref[at : at + LANES] = part.T
    rows_ref[...] = both_ref[pl.ds(pl.multiple_of((task % 2) * count, 64), count)]
    copies[1].wait()
    for step in range(tasks):
        turns_ref[step] = jnp.full((tasks, LANES), order_ref[step], jnp.int32)
    copies[2].wait()


def prepare(order, acts, own):
    tokens, depth = acts.shape
    tasks = order.shape[0]
    rows = depth // tasks
    return pl.pallas_call(
        prepare_kernel,
        out_shape=(
            jax.ShapeDtypeStruct((tokens, tokens), jnp.float32),
            jax.ShapeDtypeStruct((rows, tokens), acts.dtype),
            jax.ShapeDtypeStruct((tasks, tasks, LANES), jnp.int32),
            jax.ShapeDtypeStruct(own.shape, own.dtype),
        ),
        in_specs=[pl.BlockSpec(memory_space=pltpu.HBM)] * 3,
        out_specs=(VMEM,) * 4,
        scratch_shapes=[
            pltpu.SMEM((tasks,), jnp.int32),
            pltpu.VMEM(acts.shape, acts.dtype),
            pltpu.VMEM((2 * rows, tokens), acts.dtype),
            pltpu.SemaphoreType.DMA((3,)),
        ],
        compiler_params=params(8),
        cost_estimate=pl.CostEstimate(
            flops=2 * tokens * tokens * depth, bytes_accessed=0, transcendentals=0
        ),
        name="prepare",
    )(order, acts, own)


def place(flat_ref, offset, mine_ref, other_ref):
    core = lax.axis_index("task_1")
    base = chip_at(offset) * 2
    side = 1 - core if offset in FLIP else core
    flat_ref[base + side] = mine_ref[...]
    flat_ref[base + 1 - side] = other_ref[...]


def chip_pair(flat_ref, rows_ref, outer, first, second):
    tokens = outer.shape[0]
    first_chip, second_chip = chip_at(first), chip_at(second)
    low = 2 * jnp.minimum(first_chip, second_chip)
    high = 2 * jnp.maximum(first_chip, second_chip)
    block = lax.dot_general(
        flat_ref[pl.ds(low, 2)].reshape(2 * tokens, -1), flat_ref[pl.ds(high, 2)].reshape(2 * tokens, -1),
        (((1,), (1,)), ((), ())), preferred_element_type=jnp.float32,
    )
    for a in range(2):
        for b in range(2):
            if first == second and b < a:
                continue
            pair = block[tokens * a : tokens * (a + 1), tokens * b : tokens * (b + 1)]
            row = jnp.sum(pair * outer, axis=0, keepdims=True)
            rows_ref[high + b, pl.ds(low + a, 1), :] = row
            if first != second or a != b:
                rows_ref[low + a, pl.ds(high + b, 1), :] = row


def early_kernel(*refs):
    outer_ref, flat_ref, rows_ref = refs[-3:]
    held = (0, *ORDER[:-1])
    for at, offset in enumerate(held):
        place(flat_ref, offset, refs[2 * at], refs[2 * at + 1])
    outer = outer_ref[...]
    for at, second in enumerate(held):
        for first in held[: at + 1]:
            chip_pair(flat_ref, rows_ref, outer, first, second)


def late_kernel(flat_in_ref, rows_in_ref, m2, o2, outer_ref, row_ref, flat_ref, rows_ref):
    chips = flat_ref.shape[0] // 2
    tasks = 2 * chips
    last = ORDER[-1]
    place(flat_ref, last, m2, o2)
    outer = outer_ref[...]
    for offset in (last, 0, *ORDER[:-1]):
        chip_pair(flat_ref, rows_ref, outer, last, offset)
    lane = lax.broadcasted_iota(jnp.int32, (tasks, LANES), 1)
    sub = lax.broadcasted_iota(jnp.int32, (tasks, LANES), 0)
    gram = jnp.zeros((tasks, LANES), jnp.float32)
    for j in range(tasks):
        total = jnp.sum(rows_ref[j], axis=1, keepdims=True)
        gram = jnp.where(lane == tasks * sub + j, total, gram)
    row_ref[...] = jnp.broadcast_to(jnp.sum(gram, axis=0, keepdims=True), row_ref.shape)


def partial_gram(mine, other, outer, copies):
    tokens, width = mine[0].shape
    tasks = 2 * len(mine)
    pair_flops = 8 * tokens * tokens * width
    held = (
        jax.ShapeDtypeStruct((tasks, tokens, width), jnp.bfloat16),
        jax.ShapeDtypeStruct((tasks, tasks, LANES), jnp.float32),
    )
    flat, rows = pl.pallas_call(
        early_kernel,
        out_shape=held,
        in_specs=[VMEM] * 7,
        out_specs=(VMEM, VMEM),
        compiler_params=params(8),
        cost_estimate=pl.CostEstimate(flops=6 * pair_flops, bytes_accessed=0, transcendentals=0),
        name="early_gram",
    )(*(block[offset] for offset in (0, *ORDER[:-1]) for block in (mine, other)), outer)
    row, _, _ = pl.pallas_call(
        late_kernel,
        out_shape=(jax.ShapeDtypeStruct((copies, LANES), jnp.float32), *held),
        in_specs=[VMEM] * 5,
        out_specs=(VMEM, VMEM, VMEM),
        input_output_aliases={0: 1, 1: 2},
        compiler_params=pltpu.CompilerParams(vmem_limit_bytes=8 << 20),
        cost_estimate=pl.CostEstimate(flops=4 * pair_flops, bytes_accessed=0, transcendentals=0),
        name="late_gram",
    )(flat, rows, mine[ORDER[-1]], other[ORDER[-1]], outer)
    return row


def finish_kernel(*refs):
    chips = (len(refs) - 9) // 2
    turns_ref, grams_ref = refs[:2]
    mine, other = refs[2 : 2 + chips], refs[2 + chips : 2 + 2 * chips]
    acts_ref, update_ref, weights_ref, spread_ref, flat_ref, out_ref, sems = refs[-7:]
    core = lax.axis_index("task_1")
    _, width = mine[0].shape
    tasks = 2 * chips
    lane = lax.broadcasted_iota(jnp.int32, (tasks, LANES), 1)
    sub = lax.broadcasted_iota(jnp.int32, (tasks, LANES), 0)
    column_of = lane - tasks * sub
    gram = jnp.sum(grams_ref[...], axis=0, keepdims=True)
    gram = jnp.broadcast_to(gram, (tasks, LANES))
    mix = (lane == sub).astype(jnp.float32)
    steps = []
    for step in range(tasks):
        target = turns_ref[step]
        column = jnp.sum(jnp.where(column_of == target, gram, 0.0), axis=1, keepdims=True)
        column = jnp.broadcast_to(column, (tasks, LANES))
        scale = jnp.sum(jnp.where(sub == target, column, 0.0), axis=0, keepdims=True) + 1e-06
        steps.append((column, 1.0 / scale, (sub == target) & (lane != target)))
    for column, factor, touched in steps:
        dots = jnp.sum(mix * column, axis=0, keepdims=True)
        change = jnp.minimum(dots, 0.0) * factor
        mix = mix - jnp.where(touched, change, 0.0)
    weights = jnp.sum(jnp.where(lane < tasks, mix, 0.0), axis=1, keepdims=True)
    spread = jnp.broadcast_to(weights, (tasks, LANES))
    spread_ref[...] = spread
    flat_ref[...] = jnp.sum(jnp.where(lane == sub, spread, 0.0), axis=0)[:tasks]
    copies = [pltpu.make_async_copy(flat_ref, weights_ref, sems.at[0])]
    terms = []
    for offset in range(chips):
        base = chip_at(offset) * 2
        side = 1 - core if offset in FLIP else core
        terms.append((spread_ref[pl.ds(base + side, 1), :], mine[offset]))
        terms.append((spread_ref[pl.ds(base + 1 - side, 1), :], other[offset]))
    for start in range(0, width, 256):
        size = min(256, width - start)
        blocks = []
        for at in range(start, start + size, LANES):
            total = None
            for factor, ref in terms:
                part = factor * ref[:, at : at + LANES].astype(jnp.float32)
                total = part if total is None else total + part
            blocks.append(total.astype(jnp.bfloat16))
        cols = pl.ds(start, size)
        out_ref[:, cols] = lax.dot_general(
            acts_ref[...], jnp.concatenate(blocks, axis=1), (((1,), (0,)), ((), ())),
            preferred_element_type=jnp.float32,
        )
        copy = pltpu.make_async_copy(out_ref.at[:, cols], update_ref.at[:, cols], sems.at[len(copies)])
        copy.start()
        copies.append(copy)
    copies[0].start()
    for copy in copies:
        copy.wait()


def finish(turns, grams, mine, other, acts_rows):
    tokens, width = mine[0].shape
    tasks = 2 * len(mine)
    rows = acts_rows.shape[0]
    return pl.pallas_call(
        finish_kernel,
        out_shape=(
            jax.ShapeDtypeStruct((rows, width), jnp.float32),
            jax.ShapeDtypeStruct((tasks,), jnp.float32),
        ),
        in_specs=[VMEM] * (tasks + 3),
        out_specs=(pl.BlockSpec(memory_space=pl.ANY),) * 2,
        scratch_shapes=[
            pltpu.VMEM((tasks, LANES), jnp.float32),
            pltpu.VMEM((tasks,), jnp.float32),
            pltpu.VMEM((rows, width), jnp.float32),
            pltpu.SemaphoreType.DMA((1 + pl.cdiv(width, 256),)),
        ],
        compiler_params=pltpu.CompilerParams(vmem_limit_bytes=8 << 20),
        cost_estimate=pl.CostEstimate(
            flops=2 * rows * tokens * width, bytes_accessed=4 * rows * width, transcendentals=0
        ),
        name="finish",
    )(turns, grams, *mine, *other, acts_rows)


def moved(value, offset):
    chips = lax.axis_size("task_0")
    pairs = [
        (2 * (chip ^ offset) + (1 - core if offset in FLIP else core), 2 * chip + core)
        for chip in range(chips)
        for core in range(2)
    ]
    return lax.ppermute(value, TASK, pairs)


def farthest_first():
    rows, columns = lax.axis_size(PARAM[0]), lax.axis_size(PARAM[1])
    farthest = rows // 2 * columns + columns // 2
    return [farthest] + [chip for chip in range(rows * columns) if chip != farthest]


def shards(acts, out_grads, order):
    mine, other = [out_grads[0]], []
    for offset in (1, 2, 3):
        mine.append(moved(mine[0], offset))
    for offset in (0, 1, 2, 3):
        other.append(lax.ppermute(mine[offset], "task_1", [(0, 1), (1, 0)]))
    outer, acts_rows, turns, held = prepare(order, acts, mine[0])
    mine[0] = held
    row = partial_gram(mine, other, outer, lax.axis_size(PARAM))
    grams = lax.all_to_all(row, PARAM, 0, 0, tiled=True, axis_index_groups=[farthest_first()])
    return finish(turns, grams, mine, other, acts_rows)


def solution(mesh):
    split = Mesh(mesh.devices.reshape(4, 2, 4, 4), ("task_0", "task_1", "param_0", "param_1"))
    placed = (P(), P(TASK, None, PARAM), P())
    return jax.shard_map(
        shards, mesh=split, in_specs=placed, out_specs=(P(TASK, PARAM), P()), check_vma=False
    )
```
